32 devices in a mesh: dp: 1 (over z), m: 4 (over y), bx: 8 (over x, core).
Axes of the slice: x: 4, y: 4, z: 1, core: 2. Of those that a mesh axis runs over, the one named last changes fastest.
The devices are a block of a 4x4x8 slice.
Arguments:
- x_in: bfloat16 [24, 128, 6144], P(('dp', 'bx'), None, 'm')
- prompt_len: int32 [24], P(('dp', 'bx'))
- ln_scale: float32 [2, 6144], P(None, 'm')
- w_gate: bfloat16 [2, 6144, 8192], P(None, 'bx', 'm')
- w_up: bfloat16 [2, 6144, 8192], P(None, 'bx', 'm')
- w_q: bfloat16 [2, 6144, 48, 128], P(None, 'bx', 'm')
- w_k: bfloat16 [2, 6144, 128], P(None, 'bx')
- w_v: bfloat16 [2, 6144, 128], P(None, 'bx')
- w_down: bfloat16 [2, 8192, 6144], P(None, 'm', 'bx')
- w_o: bfloat16 [2, 48, 128, 6144], P(None, 'm', None, 'bx')
Outputs:
- output 1: bfloat16 [24, 128, 6144], P(('dp', 'bx'), None, 'm')
- output 2: bfloat16 [2, 24, 128, 128], P(None, ('dp', 'bx'))
- output 3: bfloat16 [2, 24, 128, 128], P(None, ('dp', 'bx'))
All inputs are finite; a program needn't handle non-finite values.
Results may differ from the reference program's by a relative error of at most 0.015905.
Values are sent between devices in bfloat16 or wider.
A program may use at most 768 MiB of HBM per device.

```python
import jax
import jax.numpy as jnp
from jax import lax

BATCH_ROWS = 24
SEQ_LEN = 128
EMBED_DIM = 6144
NUM_HEADS = 48
HEAD_DIM = 128
FFN_DIM = 8192
NUM_LAYERS = 2

NORM_EPS = 1e-6
ROPE_BASE = 10000.0
QUERY_BLOCK = min(SEQ_LEN, 512)
SCORE_SCALE = HEAD_DIM ** -0.5


def setup_inputs(seed: int = 0, part: int = 0) -> dict:
    base_key = jax.random.key(seed)

    def shared_normal(index, shape, fan_in):
        draw = jax.random.normal(jax.random.fold_in(base_key, index), shape, jnp.float32)
        return (draw * fan_in ** -0.5).astype(jnp.bfloat16)

    x_key = jax.random.fold_in(jax.random.fold_in(base_key, 1), part)
    x_in = jax.random.normal(x_key, (BATCH_ROWS, SEQ_LEN, EMBED_DIM), jnp.float32).astype(jnp.bfloat16)
    len_key = jax.random.fold_in(jax.random.fold_in(base_key, 2), part)
    prompt_len = jax.random.randint(len_key, (BATCH_ROWS,), SEQ_LEN // 16, SEQ_LEN + 1, dtype=jnp.int32)
    full_row = jax.random.randint(jax.random.fold_in(len_key, 1), (), 0, BATCH_ROWS)
    short_row = (full_row + jax.random.randint(jax.random.fold_in(len_key, 2), (), 1, BATCH_ROWS)) % BATCH_ROWS
    prompt_len = prompt_len.at[full_row].set(SEQ_LEN).at[short_row].set(SEQ_LEN // 16)
    ln_scale = 1.0 + 0.2 * jax.random.normal(jax.random.fold_in(base_key, 3), (NUM_LAYERS, EMBED_DIM), jnp.float32)
    return {
        'x_in': x_in,
        'prompt_len': prompt_len,
        'ln_scale': ln_scale,
        'w_gate': shared_normal(4, (NUM_LAYERS, EMBED_DIM, FFN_DIM), EMBED_DIM),
        'w_up': shared_normal(5, (NUM_LAYERS, EMBED_DIM, FFN_DIM), EMBED_DIM),
        'w_q': shared_normal(6, (NUM_LAYERS, EMBED_DIM, NUM_HEADS, HEAD_DIM), EMBED_DIM),
        'w_k': shared_normal(7, (NUM_LAYERS, EMBED_DIM, HEAD_DIM), EMBED_DIM),
        'w_v': shared_normal(8, (NUM_LAYERS, EMBED_DIM, HEAD_DIM), EMBED_DIM),
        'w_down': shared_normal(9, (NUM_LAYERS, FFN_DIM, EMBED_DIM), FFN_DIM),
        'w_o': shared_normal(10, (NUM_LAYERS, NUM_HEADS, HEAD_DIM, EMBED_DIM), NUM_HEADS * HEAD_DIM // 4),
    }


def layer_norm(x_row, scale_row):
    x_f32 = x_row.astype(jnp.float32)
    row_mean = jnp.mean(x_f32, axis=-1, keepdims=True)
    centered = x_f32 - row_mean
    row_var = jnp.mean(centered * centered, axis=-1, keepdims=True)
    return (centered * lax.rsqrt(row_var + NORM_EPS) * scale_row).astype(jnp.bfloat16)


def apply_rotary(values, cos_tab, sin_tab):
    half_dim = values.shape[-1] // 2
    first_half = values[..., :half_dim]
    second_half = values[..., half_dim:]
    return jnp.concatenate([first_half * cos_tab - second_half * sin_tab, second_half * cos_tab + first_half * sin_tab], axis=-1)


def attention_row(query_rows, key_rows, val_rows, row_len):
    block_count = SEQ_LEN // QUERY_BLOCK
    query_blocks = query_rows.reshape(block_count, QUERY_BLOCK, NUM_HEADS, HEAD_DIM)
    key_pos = jnp.arange(SEQ_LEN)
    key_f32 = key_rows.astype(jnp.float32)
    val_f32 = val_rows.astype(jnp.float32)

    def one_block(block_args):
        query_blk, block_idx = block_args
        scores = jnp.einsum('qhd,kd->hqk', query_blk.astype(jnp.float32), key_f32) * SCORE_SCALE
        query_pos = block_idx * QUERY_BLOCK + jnp.arange(QUERY_BLOCK)
        visible = (key_pos[None, :] <= query_pos[:, None]) & (key_pos[None, :] < row_len)
        scores = jnp.where(visible[None, :, :], scores, -1e30)
        attn_probs = jax.nn.softmax(scores, axis=-1).astype(jnp.bfloat16)
        block_out = jnp.einsum('hqk,kd->qhd', attn_probs.astype(jnp.float32), val_f32)
        return block_out.astype(jnp.bfloat16)

    blocks_out = lax.map(one_block, (query_blocks, jnp.arange(block_count)))
    return blocks_out.reshape(SEQ_LEN, NUM_HEADS * HEAD_DIM)


def row_forward(x_row, row_len, layer_params, cos_tab, sin_tab):
    ln_row, w_gate, w_up, w_q, w_k, w_v, w_down, w_o = layer_params
    normed = layer_norm(x_row, ln_row)
    gate_proj = jnp.dot(normed, w_gate, preferred_element_type=jnp.float32)
    up_proj = jnp.dot(normed, w_up, preferred_element_type=jnp.float32)
    act_bf = (jax.nn.silu(gate_proj) * up_proj).astype(jnp.bfloat16)
    query_lin = jnp.dot(normed, w_q.reshape(EMBED_DIM, NUM_HEADS * HEAD_DIM), preferred_element_type=jnp.float32)
    query_lin = query_lin.reshape(SEQ_LEN, NUM_HEADS, HEAD_DIM)
    query_rows = apply_rotary(query_lin, cos_tab[:, None, :], sin_tab[:, None, :]).astype(jnp.bfloat16)
    key_lin = jnp.dot(normed, w_k, preferred_element_type=jnp.float32)
    key_rows = apply_rotary(key_lin, cos_tab, sin_tab).astype(jnp.bfloat16)
    val_rows = jnp.dot(normed, w_v, preferred_element_type=jnp.float32).astype(jnp.bfloat16)
    attn_out = attention_row(query_rows, key_rows, val_rows, row_len)
    mixed_sum = jnp.dot(act_bf, w_down, preferred_element_type=jnp.float32) + jnp.dot(attn_out, w_o.reshape(NUM_HEADS * HEAD_DIM, EMBED_DIM), preferred_element_type=jnp.float32)
    y_row = (x_row.astype(jnp.float32) + mixed_sum).astype(jnp.bfloat16)
    return y_row, key_rows, val_rows


def reference(x_in, prompt_len, ln_scale, w_gate, w_up, w_q, w_k, w_v, w_down, w_o):
    half_dim = HEAD_DIM // 2
    inv_freq = ROPE_BASE ** (-jnp.arange(half_dim, dtype=jnp.float32) * (2.0 / HEAD_DIM))
    angles = jnp.arange(SEQ_LEN, dtype=jnp.float32)[:, None] * inv_freq[None, :]
    cos_tab = jnp.cos(angles)
    sin_tab = jnp.sin(angles)

    def layer_step(hidden, layer_params):
        def row_step(row_args):
            return row_forward(row_args[0], row_args[1], layer_params, cos_tab, sin_tab)
        y_rows, key_rows, val_rows = lax.map(row_step, (hidden, prompt_len))
        return y_rows, (key_rows, val_rows)

    y_out, caches = lax.scan(layer_step, x_in, (ln_scale, w_gate, w_up, w_q, w_k, w_v, w_down, w_o))
    return y_out, caches[0], caches[1]
```

```python
import jax
import jax.numpy as jnp
from jax import lax
from jax.sharding import PartitionSpec as P

NORM_EPS = 1e-6
ROPE_BASE = 10000.0


def rotary_tables(positions, head_dim):
    half_dim = head_dim // 2
    inv_freq = ROPE_BASE ** (-jnp.arange(half_dim, dtype=jnp.float32) * (2.0 / head_dim))
    angles = positions.astype(jnp.float32)[:, None] * inv_freq[None, :]
    return jnp.cos(angles), jnp.sin(angles)


def apply_rotary(values, cos_tab, sin_tab):
    half_dim = values.shape[-1] // 2
    first_half = values[..., :half_dim]
    second_half = values[..., half_dim:]
    return jnp.concatenate([first_half * cos_tab - second_half * sin_tab, second_half * cos_tab + first_half * sin_tab], axis=-1)


def masked_attention(queries, key_rows, val_rows, positions, row_lens):
    score_scale = queries.shape[-1] ** -0.5
    scores = jnp.einsum('bthd,bsd->bhts', queries, key_rows, preferred_element_type=jnp.float32) * score_scale
    visible = (positions[None, None, None, :] <= positions[None, None, :, None]) & (positions[None, None, None, :] < row_lens[:, None, None, None])
    scores = jnp.where(visible, scores, -1e30)
    attn_probs = jax.nn.softmax(scores, axis=-1).astype(jnp.bfloat16)
    return jnp.einsum('bhts,bsd->bthd', attn_probs, val_rows, preferred_element_type=jnp.float32).astype(jnp.bfloat16)


class Pairing:
    def __init__(self, bx_size, first):
        chips = bx_size // 2
        self.partner = [0] * chips
        for low in range(first, first + chips, 2):
            a, b = low % chips, (low + 1) % chips
            self.partner[a], self.partner[b] = b, a
        self.perm = [(2 * c + k, 2 * self.partner[c] + k) for c in range(chips) for k in range(2)]

    def send(self, value):
        return lax.ppermute(value, 'bx', self.perm)


def solution(mesh):
    m_size = mesh.shape['m']
    bx_size = mesh.shape['bx']
    chips = bx_size // 2
    batch_axes = ('dp', 'bx')
    row_spec = P(batch_axes, None, 'm')
    cache_spec = P(None, batch_axes, None, None)
    in_specs = (row_spec, P(batch_axes), P(None, 'm'), P(None, 'bx', 'm'), P(None, 'bx', 'm'), P(None, 'bx', 'm', None), P(None, 'bx', None), P(None, 'bx', None), P(None, 'm', 'bx'), P(None, 'm', None, 'bx'))
    pairings = (Pairing(bx_size, 0), Pairing(bx_size, 1))
    core_perm = [(i, i ^ 1) for i in range(bx_size)]

    def swap_core(value):
        return lax.ppermute(value, 'bx', core_perm)

    def device_program(x_in, prompt_len, ln_scale, w_gate, w_up, w_q, w_k, w_v, w_down, w_o):
        rows, seq, feat = x_in.shape
        head_dim = w_k.shape[-1]
        embed_dim = feat * m_size
        e_chip = embed_dim // chips
        me = lax.axis_index('bx')
        chip, core = me // 2, me % 2
        positions = jnp.arange(seq)
        cos_tab, sin_tab = rotary_tables(positions, head_dim)
        kv_w = lax.all_gather(jnp.concatenate([w_k, w_v], axis=2), 'bx', axis=1, tiled=True)

        def spread(w, e_axis, same_col, same_row, c_index, partners):
            f_axis = 1 - e_axis
            half = w.shape[f_axis] // 2
            take = lambda v, i: lax.dynamic_slice_in_dim(v, i * (v.shape[f_axis] // 2), v.shape[f_axis] // 2, f_axis)
            mine = take(w, core)
            other = swap_core(take(w, 1 - core))
            mine_c = jnp.concatenate([take(mine, c_index), take(other, c_index)], axis=e_axis)
            other_c = jnp.concatenate([take(mine, 1 - c_index), take(other, 1 - c_index)], axis=e_axis)
            from_row = same_row.send(other_c)
            far = [same_col.send(mine_c), same_col.send(from_row)]
            pieces = [mine_c, from_row] + far
            shape = [half // 2, half // 2]
            shape[e_axis] = embed_dim
            full = jnp.zeros(shape, w.dtype)
            block = e_chip // 2
            for piece, owner in zip(pieces, partners):
                for j in range(2):
                    sub = lax.slice_in_dim(piece, j * block, (j + 1) * block, axis=e_axis)
                    full = lax.dynamic_update_slice_in_dim(full, sub, (2 * owner + (core + j) % 2) * block, e_axis)
            return full

        hidden = x_in.reshape(rows * seq, feat)
        k_layers = []
        v_layers = []
        weights = []
        for layer_idx in range(w_gate.shape[0]):
            same_col = pairings[layer_idx % 2]
            same_row = pairings[(layer_idx + 1) % 2]
            c_index = ((chip + layer_idx % 2) // 2) % 2
            row_p = jnp.asarray(same_row.partner, jnp.int32)[chip]
            col_p = jnp.asarray(same_col.partner, jnp.int32)[chip]
            far_p = jnp.asarray(same_row.partner, jnp.int32)[col_p]
            partners = (chip, row_p, col_p, far_p)
            args = (same_col, same_row, c_index, partners)
            heads = w_q.shape[2]
            gate = spread(w_gate[layer_idx], 0, *args)
            up = spread(w_up[layer_idx], 0, *args)
            query_w = spread(w_q[layer_idx].reshape(w_q.shape[1], heads * head_dim), 0, *args)
            down = spread(w_down[layer_idx], 1, *args)
            out_w = spread(w_o[layer_idx].reshape(heads * head_dim, w_o.shape[-1]), 1, *args)
            weights.append((same_row, gate, up, query_w, down, out_w))

        for layer_idx in range(w_gate.shape[0]):
            same_row, gate, up, query_w, down, out_w = weights[layer_idx]
            hidden_f32 = hidden.astype(jnp.float32)
            moments = jnp.stack([jnp.sum(hidden_f32, axis=-1), jnp.sum(hidden_f32 * hidden_f32, axis=-1)])
            moments = lax.psum(moments, 'm')
            row_mean = (moments[0] / embed_dim)[..., None]
            row_var = (moments[1] / embed_dim)[..., None] - row_mean * row_mean
            normed = ((hidden_f32 - row_mean) * lax.rsqrt(row_var + NORM_EPS) * ln_scale[layer_idx]).astype(jnp.bfloat16)
            normed = jnp.concatenate([normed, same_row.send(normed)], axis=0)
            normed = lax.all_gather(normed, 'm', axis=1, tiled=True)
            normed = jnp.concatenate([normed, swap_core(normed)], axis=0)
            lens = jnp.concatenate([prompt_len, same_row.send(prompt_len)])
            lens = jnp.concatenate([lens, swap_core(lens)])
            total = normed.shape[0]
            batch = total // seq

            gate_proj = jnp.dot(normed, gate, preferred_element_type=jnp.float32)
            up_proj = jnp.dot(normed, up, preferred_element_type=jnp.float32)
            act_bf = (jax.nn.silu(gate_proj) * up_proj).astype(jnp.bfloat16)
            query_lin = jnp.dot(normed, query_w, preferred_element_type=jnp.float32).reshape(batch, seq, -1, head_dim)
            queries = apply_rotary(query_lin, cos_tab[:, None, :], sin_tab[:, None, :]).astype(jnp.bfloat16)
            kv_lin = jnp.dot(normed, kv_w[layer_idx], preferred_element_type=jnp.float32).reshape(batch, seq, 2 * head_dim)
            key_rows = apply_rotary(kv_lin[..., :head_dim], cos_tab, sin_tab).astype(jnp.bfloat16)
            val_rows = kv_lin[..., head_dim:].astype(jnp.bfloat16)
            attn_out = masked_attention(queries, key_rows, val_rows, positions, lens).reshape(total, -1)

            both = jnp.concatenate([act_bf, attn_out], axis=1)
            both_w = jnp.concatenate([down, out_w], axis=0)
            partial = jnp.dot(both, both_w, preferred_element_type=jnp.float32).astype(jnp.bfloat16)
            from_core = swap_core(partial[total // 2:])
            partial = (partial[:total // 2].astype(jnp.float32) + from_core.astype(jnp.float32)).astype(jnp.bfloat16)
            reduced = lax.psum_scatter(partial, 'm', scatter_dimension=1, tiled=True)
            from_row = same_row.send(reduced[total // 4:])
            hidden = (hidden_f32 + reduced[:total // 4].astype(jnp.float32) + from_row.astype(jnp.float32)).astype(jnp.bfloat16)
            k_layers.append(key_rows[:rows])
            v_layers.append(val_rows[:rows])
        return hidden.reshape(rows, seq, feat), jnp.stack(k_layers), jnp.stack(v_layers)

    return jax.shard_map(device_program, mesh=mesh, in_specs=in_specs, out_specs=(row_spec, cache_spec, cache_spec), check_vma=False)
```

```python
import functools

import jax
import jax.numpy as jnp
from jax import lax
from jax.experimental import pallas as pl
from jax.experimental.pallas import tpu as pltpu
from jax.sharding import PartitionSpec as P


NORM_EPS = 1e-6
ROPE_BASE = 10000.0


def rotary_tables(positions, head_dim):
    half_dim = head_dim // 2
    inv_freq = ROPE_BASE ** (-jnp.arange(half_dim, dtype=jnp.float32) * (2.0 / head_dim))
    angles = positions.astype(jnp.float32)[:, None] * inv_freq[None, :]
    return jnp.cos(angles), jnp.sin(angles)


def up_kernel(head_dim, order_ref, lens_ref, mine_ref, other_ref, scale_ref, cos_ref, sin_ref, *refs):
    weights, (both_ref, k_ref, v_ref, h_ref, q_ref, keys_ref, vals_ref, wg_ref, wu_ref, wq_ref, wv_ref, sems) = refs[:16], refs[16:]
    copies = []
    for i, (group, dst) in enumerate(zip((weights[0:4], weights[4:8], weights[8:12], weights[12:16]), (wg_ref, wu_ref, wq_ref, wv_ref))):
        for p, src in enumerate(group):
            if dst is wq_ref:
                for h in range(src.shape[0]):
                    copies.append(pltpu.make_async_copy(src.at[h], dst.at[p, :, pl.ds(h * head_dim, head_dim)], sems.at[i, p]))
            else:
                copies.append(pltpu.make_async_copy(src, dst.at[p], sems.at[i, p]))
    for copy in copies:
        copy.start()

    blocks, half_rows, feat = mine_ref.shape
    embed_dim = blocks * feat
    part = feat // 2
    step = 16

    def norm(i, carry):
        rows = pl.ds(pl.multiple_of(i * step, step), step)
        for src, base in ((mine_ref, 0), (other_ref, half_rows)):
            xs = [src[e, rows, :].astype(jnp.float32) for e in range(blocks)]
            mean = sum(jnp.sum(x, axis=-1, keepdims=True) for x in xs) / embed_dim
            xs = [x - mean for x in xs]
            var = sum(jnp.sum(x * x, axis=-1, keepdims=True) for x in xs) / embed_dim
            inv = lax.rsqrt(var + NORM_EPS)
            out_rows = pl.ds(pl.multiple_of(base + i * step, step), step)
            for e in range(blocks):
                y = (xs[e] * inv * scale_ref[e:e + 1, :]).astype(jnp.bfloat16)
                h_ref[2 * e, out_rows, :] = y[:, :part]
                h_ref[2 * e + 1, out_rows, :] = y[:, part:]
        return carry

    lax.fori_loop(0, half_rows // step, norm, 0)
    for copy in copies:
        copy.wait()

    n_parts = 2 * blocks
    order = [order_ref[p] for p in range(n_parts)]
    tile = 256
    f_cols = wg_ref.shape[-1]
    n_heads = wq_ref.shape[-1] // head_dim
    half_dim = head_dim // 2

    def product(rows, w_ref, cols):
        total = None
        for p in range(n_parts):
            w = w_ref[p // 2, pl.ds((p % 2) * part, part), cols]
            term = jnp.dot(h_ref[order[p], rows, :], w, preferred_element_type=jnp.float32)
            total = term if total is None else total + term
        return total

    def project(r, carry):
        rows = pl.ds(pl.multiple_of(r * tile, tile), tile)
        for n in range(0, f_cols, tile):
            cols = pl.ds(n, tile)
            gate = product(rows, wg_ref, cols)
            up = product(rows, wu_ref, cols)
            both_ref[rows, cols] = (gate * (1.0 / (1.0 + jnp.exp(-gate))) * up).astype(jnp.bfloat16)
        cos_t = jnp.concatenate([cos_ref[...]] * (tile // cos_ref.shape[0]), axis=0)
        sin_t = jnp.concatenate([sin_ref[...]] * (tile // sin_ref.shape[0]), axis=0)
        rotary = lambda u: (u * cos_t + pltpu.roll(u, half_dim, 1) * sin_t).astype(jnp.bfloat16)
        kv = product(rows, wv_ref, pl.ds(0, 2 * head_dim))
        keys_ref[rows, :] = rotary(kv[:, :head_dim])
        vals_ref[rows, :] = kv[:, head_dim:].astype(jnp.bfloat16)
        query = product(rows, wq_ref, pl.ds(0, n_heads * head_dim))
        for h in range(n_heads):
            cols = slice(h * head_dim, (h + 1) * head_dim)
            q_ref[rows, cols] = rotary(query[:, cols])
        return carry

    lax.fori_loop(0, h_ref.shape[1] // tile, project, 0)
    seq = cos_ref.shape[0]
    k_ref[...] = keys_ref[:seq, :]
    v_ref[...] = vals_ref[:seq, :]
    row_id = lax.broadcasted_iota(jnp.int32, (seq, seq), 0)
    col_id = lax.broadcasted_iota(jnp.int32, (seq, seq), 1)

    def attend(b, carry):
        rows = pl.ds(pl.multiple_of(b * seq, seq), seq)
        keys, vals = keys_ref[rows, :], vals_ref[rows, :]
        visible = (col_id <= row_id) & (col_id < lens_ref[b])
        for h in range(n_heads):
            query = q_ref[rows, h * head_dim:(h + 1) * head_dim]
            scores = lax.dot_general(query, keys, (((1,), (1,)), ((), ())), preferred_element_type=jnp.float32) * (head_dim ** -0.5)
            scores = jnp.where(visible, scores, -1e30)
            weight = jnp.exp(scores - jnp.max(scores, axis=-1, keepdims=True))
            probs = (weight / jnp.sum(weight, axis=-1, keepdims=True)).astype(jnp.bfloat16)
            out = jnp.dot(probs, vals, preferred_element_type=jnp.float32)
            both_ref[rows, f_cols + h * head_dim:f_cols + (h + 1) * head_dim] = out.astype(jnp.bfloat16)
        return carry

    lax.fori_loop(0, h_ref.shape[1] // seq, attend, 0)


def down_kernel(order_ref, both_ref, *refs):
    weights, (keep_ref, send_ref, w_ref, sems) = refs[:8], refs[8:]
    pieces = w_ref.shape[0]
    copies = []
    for p in range(pieces):
        depth = weights[p].shape[0]
        copies.append((
            pltpu.make_async_copy(weights[p], w_ref.at[p, pl.ds(0, depth), :], sems.at[0, p]),
            pltpu.make_async_copy(weights[pieces + p], w_ref.at[p, pl.ds(depth, weights[pieces + p].shape[0]), :], sems.at[1, p]),
        ))
    for pair in copies:
        for copy in pair:
            copy.start()
    half_rows = keep_ref.shape[1]
    part = w_ref.shape[-1] // 2
    tile = 256
    for p in range(pieces):
        for copy in copies[p]:
            copy.wait()
        for j in range(2):
            block = order_ref[2 * p + j]
            for n in range(0, part, tile):
                w = w_ref[p, :, j * part + n:j * part + n + tile]
                cols = pl.ds(pl.multiple_of(lax.rem(block, 2) * part + n, 128), tile)
                for dst, base in ((send_ref, half_rows), (keep_ref, 0)):
                    out = jnp.dot(both_ref[base:base + half_rows, :], w, preferred_element_type=jnp.float32)
                    dst[lax.div(block, 2), :, cols] = out.astype(jnp.bfloat16)


def up_call(order, lens, mine, other, scale, cos_t, sin_t, gate, up, query, kv):
    blocks, half_rows, feat = mine.shape
    rows = 2 * half_rows
    head_dim = cos_t.shape[-1]
    f_cols, heads = gate[0].shape[-1], query[0].shape[0]
    wide = f_cols + heads * head_dim
    n_all = 2 * f_cols + (heads + 2) * head_dim
    vmem, smem, hbm = (pl.BlockSpec(memory_space=space) for space in (pltpu.VMEM, pltpu.SMEM, pltpu.HBM))
    bf16 = jnp.bfloat16
    return pl.pallas_call(
        functools.partial(up_kernel, head_dim),
        out_shape=(jax.ShapeDtypeStruct((rows, wide), bf16), jax.ShapeDtypeStruct(cos_t.shape, bf16), jax.ShapeDtypeStruct(cos_t.shape, bf16)),
        in_specs=[smem, smem] + [vmem] * 5 + [hbm] * 16,
        out_specs=(vmem, vmem, vmem),
        scratch_shapes=[
            pltpu.VMEM((2 * blocks, rows, feat // 2), bf16),
            pltpu.VMEM((rows, heads * head_dim), bf16),
            pltpu.VMEM((rows, head_dim), bf16),
            pltpu.VMEM((rows, head_dim), bf16),
            pltpu.VMEM((blocks, feat, f_cols), bf16),
            pltpu.VMEM((blocks, feat, f_cols), bf16),
            pltpu.VMEM((blocks, feat, heads * head_dim), bf16),
            pltpu.VMEM((blocks, feat, 2 * head_dim), bf16),
            pltpu.SemaphoreType.DMA((4, blocks)),
        ],
        compiler_params=pltpu.CompilerParams(vmem_limit_bytes=60 << 20),
        cost_estimate=pl.CostEstimate(flops=2 * rows * blocks * feat * n_all, bytes_accessed=2 * blocks * feat * (n_all + rows), transcendentals=0),
    )(order, lens, mine, other, scale, cos_t, sin_t, *gate, *up, *query, *kv)


def down_call(order, both, down, out_w):
    rows, wide = both.shape
    pieces, feat = len(down), down[0].shape[-1]
    vmem, smem, hbm = (pl.BlockSpec(memory_space=space) for space in (pltpu.VMEM, pltpu.SMEM, pltpu.HBM))
    shape = jax.ShapeDtypeStruct((pieces, rows // 2, feat), jnp.bfloat16)
    return pl.pallas_call(
        down_kernel,
        out_shape=(shape, shape),
        in_specs=[smem, vmem] + [hbm] * (2 * pieces),
        out_specs=(vmem, vmem),
        scratch_shapes=[pltpu.VMEM((pieces, wide, feat), jnp.bfloat16), pltpu.SemaphoreType.DMA((2, pieces))],
        compiler_params=pltpu.CompilerParams(vmem_limit_bytes=48 << 20),
        cost_estimate=pl.CostEstimate(flops=2 * rows * wide * pieces * feat, bytes_accessed=2 * pieces * feat * (wide + rows), transcendentals=0),
    )(order, both, *down, *out_w)


class Pairing:
    def __init__(self, bx_size, first):
        chips = bx_size // 2
        self.partner = [0] * chips
        for low in range(first, first + chips, 2):
            a, b = low % chips, (low + 1) % chips
            self.partner[a], self.partner[b] = b, a
        self.perm = [(2 * c + k, 2 * self.partner[c] + k) for c in range(chips) for k in range(2)]

    def send(self, value):
        return lax.ppermute(value, 'bx', self.perm)


def solution(mesh):
    bx_size = mesh.shape['bx']
    batch_axes = ('dp', 'bx')
    row_spec = P(batch_axes, None, 'm')
    cache_spec = P(None, batch_axes, None, None)
    in_specs = (row_spec, P(batch_axes), P(None, 'm'), P(None, 'bx', 'm'), P(None, 'bx', 'm'), P(None, 'bx', 'm', None), P(None, 'bx', None), P(None, 'bx', None), P(None, 'm', 'bx'), P(None, 'm', None, 'bx'))
    pairings = (Pairing(bx_size, 0), Pairing(bx_size, 1))
    core_perm = [(i, i ^ 1) for i in range(bx_size)]

    def swap_core(value):
        return lax.ppermute(value, 'bx', core_perm)

    def device_program(x_in, prompt_len, ln_scale, w_gate, w_up, w_q, w_k, w_v, w_down, w_o):
        rows, seq, _ = x_in.shape
        head_dim = w_k.shape[-1]
        me = lax.axis_index('bx').astype(jnp.uint32)
        chip, core = me >> 1, me & 1
        positions = jnp.arange(seq)
        cos_tab, sin_tab = rotary_tables(positions, head_dim)
        cos_full = jnp.concatenate([cos_tab, cos_tab], axis=1)
        sin_full = jnp.concatenate([-sin_tab, sin_tab], axis=1)
        scale_all = lax.all_gather(ln_scale, 'm', axis=0)
        layers = w_gate.shape[0]
        heads = w_q.shape[2]

        def spread(w, e_axis, layer, same_col, same_row, c_index):
            f_axis = 1 - e_axis
            half = w.shape[1 + f_axis] // 2
            quarter = half // 2

            def take(at, size):
                starts, sizes = [jnp.uint32(layer), jnp.uint32(0), jnp.uint32(0)], list(w.shape[1:3])
                starts[1 + f_axis], sizes[f_axis] = at * size, size
                tail = w.shape[3:]
                starts += [jnp.uint32(0)] * len(tail)
                return lax.dynamic_slice(w, starts, [1] + sizes + list(tail))[0]

            other = swap_core(take(1 - core, half))
            other_at = lambda i: lax.dynamic_slice_in_dim(other, i * quarter, quarter, f_axis)
            mine_c = jnp.concatenate([take(2 * core + c_index, quarter), other_at(c_index)], axis=e_axis)
            other_c = jnp.concatenate([take(2 * core + (1 - c_index), quarter), other_at(1 - c_index)], axis=e_axis)
            from_row = same_row.send(other_c)
            return [mine_c, from_row, same_col.send(mine_c), same_col.send(from_row)]

        def spread_kv(w, same_col, same_row):
            from_row = same_row.send(w)
            mine = jnp.stack([w, from_row, same_col.send(w), same_col.send(from_row)])
            full = jnp.concatenate([mine, swap_core(mine)], axis=1)
            return [full[i] for i in range(4)]

        plans = []
        for layer in range(layers):
            same_col = pairings[layer % 2]
            same_row = pairings[(layer + 1) % 2]
            flipped = layer % 2
            c_index = ((chip + flipped) >> 1) & 1
            owners = tuple(chip ^ mask for mask in ((0, 3, 1, 2), (0, 1, 3, 2))[flipped])
            order = jnp.stack([2 * owner + (core ^ j) for owner in owners for j in range(2)]).astype(jnp.int32)
            args = (same_col, same_row, c_index)
            gate = spread(w_gate, 0, layer, *args)
            up = spread(w_up, 0, layer, *args)
            query_w = spread(jnp.swapaxes(w_q, 1, 2), 1, layer, *args)
            kv_w = spread_kv(jnp.concatenate([w_k[layer], w_v[layer]], axis=1), same_col, same_row)
            down = spread(w_down, 1, layer, *args)
            out_w = spread(w_o.reshape(layers, heads * head_dim, w_o.shape[-1]), 1, layer, *args)
            lens = jnp.stack([prompt_len, same_row.send(prompt_len)])
            lens = jnp.stack([lens, swap_core(lens)])
            plans.append((same_row, order, lens, gate, up, query_w, kv_w, down, out_w))

        hidden = [lax.optimization_barrier(x_in[c]) for c in range(rows)]
        k_layers = []
        v_layers = []
        for layer in range(layers):
            same_row, order, lens, gate, up, query_w, kv_w, down, out_w = plans[layer]
            k_rows, v_rows, following = [], [], []
            for c in range(rows):
                shared = same_row.send(hidden[c])
                pair = jnp.concatenate([hidden[c], shared], axis=0)
                mine = lax.all_gather(pair, 'm', axis=0)
                other = swap_core(mine)
                both, key_rows, val_rows = up_call(order, lens[:, :, c].reshape(-1), mine, other, scale_all[:, layer], cos_full, sin_full, gate, up, query_w, kv_w)
                k_rows.append(key_rows)
                v_rows.append(val_rows)
                keep, send = down_call(order, both, down, out_w)
                from_core = swap_core(send)
                ordered = (keep.astype(jnp.float32) + from_core.astype(jnp.float32)).astype(jnp.bfloat16)
                reduced = lax.psum_scatter(ordered, 'm', scatter_dimension=0)
                from_row = same_row.send(reduced[seq:])
                following.append((hidden[c].astype(jnp.float32) + (reduced[:seq].astype(jnp.float32) + from_row.astype(jnp.float32))).astype(jnp.bfloat16))
            hidden = following
            k_layers.append(jnp.stack(k_rows))
            v_layers.append(jnp.stack(v_rows))
        return jnp.stack(hidden), jnp.stack(k_layers), jnp.stack(v_layers)

    return jax.shard_map(device_program, mesh=mesh, in_specs=in_specs, out_specs=(row_spec, cache_spec, cache_spec), check_vma=False)
```

```python
import functools

import jax
import jax.numpy as jnp
from jax import lax
from jax.experimental import pallas as pl
from jax.experimental.pallas import tpu as pltpu
from jax.sharding import PartitionSpec as P


NORM_EPS = 1e-6
ROPE_BASE = 10000.0


def rotary_tables(positions, head_dim):
    half_dim = head_dim // 2
    inv_freq = ROPE_BASE ** (-jnp.arange(half_dim, dtype=jnp.float32) * (2.0 / head_dim))
    angles = positions.astype(jnp.float32)[:, None] * inv_freq[None, :]
    return jnp.cos(angles), jnp.sin(angles)


def up_kernel(head_dim, order_ref, lens_ref, mine_ref, other_ref, scale_ref, cos_ref, sin_ref, *refs):
    weights, (both_ref, k_ref, v_ref, h_ref, q_ref, keys_ref, vals_ref, wg_ref, wu_ref, wq_ref, wv_ref, sems) = refs[:16], refs[16:]
    copies = []
    for i, (group, dst) in enumerate(zip((weights[0:4], weights[4:8], weights[8:12], weights[12:16]), (wg_ref, wu_ref, wq_ref, wv_ref))):
        for p, src in enumerate(group):
            if dst is wq_ref:
                for h in range(src.shape[0]):
                    copies.append(pltpu.make_async_copy(src.at[h], dst.at[p, :, pl.ds(h * head_dim, head_dim)], sems.at[i, p]))
            else:
                copies.append(pltpu.make_async_copy(src, dst.at[p], sems.at[i, p]))
    for copy in copies:
        copy.start()

    blocks, half_rows, feat = mine_ref.shape
    embed_dim = blocks * feat
    part = feat // 2
    step = 16

    def norm(i, carry):
        rows = pl.ds(pl.multiple_of(i * step, step), step)
        for src, base in ((mine_ref, 0), (other_ref, half_rows)):
            xs = [src[e, rows, :].astype(jnp.float32) for e in range(blocks)]
            mean = sum(jnp.sum(x, axis=-1, keepdims=True) for x in xs) / embed_dim
            xs = [x - mean for x in xs]
            var = sum(jnp.sum(x * x, axis=-1, keepdims=True) for x in xs) / embed_dim
            inv = lax.rsqrt(var + NORM_EPS)
            out_rows = pl.ds(pl.multiple_of(base + i * step, step), step)
            for e in range(blocks):
                y = (xs[e] * inv * scale_ref[e:e + 1, :]).astype(jnp.bfloat16)
                h_ref[2 * e, out_rows, :] = y[:, :part]
                h_ref[2 * e + 1, out_rows, :] = y[:, part:]
        return carry

    lax.fori_loop(0, half_rows // step, norm, 0)
    early = 2 * blocks
    for copy in copies[:early]:
        copy.wait()

    n_parts = 2 * blocks
    order = [order_ref[p] for p in range(n_parts)]
    tile = 256
    f_cols = wg_ref.shape[-1]
    n_heads = wq_ref.shape[-1] // head_dim
    half_dim = head_dim // 2

    def product(rows, w_ref, cols):
        total = None
        for p in range(n_parts):
            w = w_ref[p // 2, pl.ds((p % 2) * part, part), cols]
            term = jnp.dot(h_ref[order[p], rows, :], w, preferred_element_type=jnp.float32)
            total = term if total is None else total + term
        return total

    n_cols = f_cols // tile

    def project_ffn(i, carry):
        rows = pl.ds(pl.multiple_of(lax.div(i, n_cols) * tile, tile), tile)
        cols = pl.ds(pl.multiple_of(lax.rem(i, n_cols) * tile, tile), tile)
        gate = product(rows, wg_ref, cols)
        up = product(rows, wu_ref, cols)
        both_ref[rows, cols] = (gate * (1.0 / (1.0 + jnp.exp(-gate))) * up).astype(jnp.bfloat16)
        return carry

    lax.fori_loop(0, h_ref.shape[1] // tile * n_cols, project_ffn, 0)
    for copy in copies[early:]:
        copy.wait()

    def project(r, carry):
        rows = pl.ds(pl.multiple_of(r * tile, tile), tile)
        cos_t = jnp.concatenate([cos_ref[...]] * (tile // cos_ref.shape[0]), axis=0)
        sin_t = jnp.concatenate([sin_ref[...]] * (tile // sin_ref.shape[0]), axis=0)
        rotary = lambda u: (u * cos_t + pltpu.roll(u, half_dim, 1) * sin_t).astype(jnp.bfloat16)
        kv = product(rows, wv_ref, pl.ds(0, 2 * head_dim))
        keys_ref[rows, :] = rotary(kv[:, :head_dim])
        vals_ref[rows, :] = kv[:, head_dim:].astype(jnp.bfloat16)
        query = product(rows, wq_ref, pl.ds(0, n_heads * head_dim))
        for h in range(n_heads):
            cols = slice(h * head_dim, (h + 1) * head_dim)
            q_ref[rows, cols] = rotary(query[:, cols])
        return carry

    lax.fori_loop(0, h_ref.shape[1] // tile, project, 0)
    seq = cos_ref.shape[0]
    k_ref[...] = keys_ref[:seq, :]
    v_ref[...] = vals_ref[:seq, :]
    row_id = lax.broadcasted_iota(jnp.int32, (seq, seq), 0)
    col_id = lax.broadcasted_iota(jnp.int32, (seq, seq), 1)

    def attend(b, carry):
        rows = pl.ds(pl.multiple_of(b * seq, seq), seq)
        keys, vals = keys_ref[rows, :], vals_ref[rows, :]
        visible = (col_id <= row_id) & (col_id < lens_ref[b])
        for h in range(n_heads):
            query = q_ref[rows, h * head_dim:(h + 1) * head_dim]
            scores = lax.dot_general(query, keys, (((1,), (1,)), ((), ())), preferred_element_type=jnp.float32) * (head_dim ** -0.5)
            scores = jnp.where(visible, scores, -1e30)
            weight = jnp.exp(scores - jnp.max(scores, axis=-1, keepdims=True))
            probs = (weight / jnp.sum(weight, axis=-1, keepdims=True)).astype(jnp.bfloat16)
            out = jnp.dot(probs, vals, preferred_element_type=jnp.float32)
            both_ref[rows, f_cols + h * head_dim:f_cols + (h + 1) * head_dim] = out.astype(jnp.bfloat16)
        return carry

    lax.fori_loop(0, h_ref.shape[1] // seq, attend, 0)


def down_kernel(order_ref, both_ref, *refs):
    weights, (keep_ref, send_ref, w_ref, sems) = refs[:8], refs[8:]
    pieces = w_ref.shape[0]
    copies = []
    for p in range(pieces):
        depth = weights[p].shape[0]
        copies.append((
            pltpu.make_async_copy(weights[p], w_ref.at[p, pl.ds(0, depth), :], sems.at[0, p]),
            pltpu.make_async_copy(weights[pieces + p], w_ref.at[p, pl.ds(depth, weights[pieces + p].shape[0]), :], sems.at[1, p]),
        ))
    for pair in copies:
        for copy in pair:
            copy.start()
    half_rows = keep_ref.shape[1]
    part = w_ref.shape[-1] // 2
    tile = 256

    def piece(p, carry):
        for i, first in enumerate((0, pieces)):
            depth = weights[first].shape[0]
            start = i * weights[0].shape[0]
            pltpu.make_async_copy(weights[first], w_ref.at[p, pl.ds(start, depth), :], sems.at[i, p]).wait()
        for j in range(2):
            block = order_ref[2 * p + j]
            for n in range(0, part, tile):
                w = w_ref[p, :, j * part + n:j * part + n + tile]
                cols = pl.ds(pl.multiple_of(lax.rem(block, 2) * part + n, 128), tile)
                for dst, base in ((send_ref, half_rows), (keep_ref, 0)):
                    out = jnp.dot(both_ref[base:base + half_rows, :], w, preferred_element_type=jnp.float32)
                    dst[lax.div(block, 2), :, cols] = out.astype(jnp.bfloat16)
        return carry

    lax.fori_loop(0, pieces, piece, 0)


def up_call(order, lens, mine, other, scale, cos_t, sin_t, gate, up, query, kv):
    blocks, half_rows, feat = mine.shape
    rows = 2 * half_rows
    head_dim = cos_t.shape[-1]
    f_cols, heads = gate[0].shape[-1], query[0].shape[0]
    wide = f_cols + heads * head_dim
    n_all = 2 * f_cols + (heads + 2) * head_dim
    vmem, smem, hbm = (pl.BlockSpec(memory_space=space) for space in (pltpu.VMEM, pltpu.SMEM, pltpu.HBM))
    bf16 = jnp.bfloat16
    return pl.pallas_call(
        functools.partial(up_kernel, head_dim),
        out_shape=(jax.ShapeDtypeStruct((rows, wide), bf16), jax.ShapeDtypeStruct(cos_t.shape, bf16), jax.ShapeDtypeStruct(cos_t.shape, bf16)),
        in_specs=[smem, smem] + [vmem] * 5 + [hbm] * 16,
        out_specs=(vmem, vmem, vmem),
        scratch_shapes=[
            pltpu.VMEM((2 * blocks, rows, feat // 2), bf16),
            pltpu.VMEM((rows, heads * head_dim), bf16),
            pltpu.VMEM((rows, head_dim), bf16),
            pltpu.VMEM((rows, head_dim), bf16),
            pltpu.VMEM((blocks, feat, f_cols), bf16),
            pltpu.VMEM((blocks, feat, f_cols), bf16),
            pltpu.VMEM((blocks, feat, heads * head_dim), bf16),
            pltpu.VMEM((blocks, feat, 2 * head_dim), bf16),
            pltpu.SemaphoreType.DMA((4, blocks)),
        ],
        compiler_params=pltpu.CompilerParams(vmem_limit_bytes=60 << 20),
        cost_estimate=pl.CostEstimate(flops=2 * rows * blocks * feat * n_all, bytes_accessed=2 * blocks * feat * (n_all + rows), transcendentals=0),
    )(order, lens, mine, other, scale, cos_t, sin_t, *gate, *up, *query, *kv)


def down_call(order, both, down, out_w):
    rows, wide = both.shape
    pieces, feat = len(down), down[0].shape[-1]
    vmem, smem, hbm = (pl.BlockSpec(memory_space=space) for space in (pltpu.VMEM, pltpu.SMEM, pltpu.HBM))
    shape = jax.ShapeDtypeStruct((pieces, rows // 2, feat), jnp.bfloat16)
    return pl.pallas_call(
        down_kernel,
        out_shape=(shape, shape),
        in_specs=[smem, vmem] + [hbm] * (2 * pieces),
        out_specs=(vmem, vmem),
        scratch_shapes=[pltpu.VMEM((pieces, wide, feat), jnp.bfloat16), pltpu.SemaphoreType.DMA((2, pieces))],
        compiler_params=pltpu.CompilerParams(vmem_limit_bytes=48 << 20),
        cost_estimate=pl.CostEstimate(flops=2 * rows * wide * pieces * feat, bytes_accessed=2 * pieces * feat * (wide + rows), transcendentals=0),
    )(order, both, *down, *out_w)


class Pairing:
    def __init__(self, bx_size, first):
        chips = bx_size // 2
        self.partner = [0] * chips
        for low in range(first, first + chips, 2):
            a, b = low % chips, (low + 1) % chips
            self.partner[a], self.partner[b] = b, a
        self.perm = [(2 * c + k, 2 * self.partner[c] + k) for c in range(chips) for k in range(2)]

    def send(self, value):
        return lax.ppermute(value, 'bx', self.perm)


def solution(mesh):
    bx_size = mesh.shape['bx']
    batch_axes = ('dp', 'bx')
    row_spec = P(batch_axes, None, 'm')
    cache_spec = P(None, batch_axes, None, None)
    in_specs = (row_spec, P(batch_axes), P(None, 'm'), P(None, 'bx', 'm'), P(None, 'bx', 'm'), P(None, 'bx', 'm', None), P(None, 'bx', None), P(None, 'bx', None), P(None, 'm', 'bx'), P(None, 'm', None, 'bx'))
    pairings = (Pairing(bx_size, 0), Pairing(bx_size, 1))
    core_perm = [(i, i ^ 1) for i in range(bx_size)]

    def swap_core(value):
        return lax.ppermute(value, 'bx', core_perm)

    def device_program(x_in, prompt_len, ln_scale, w_gate, w_up, w_q, w_k, w_v, w_down, w_o):
        rows, seq, _ = x_in.shape
        head_dim = w_k.shape[-1]
        me = lax.axis_index('bx').astype(jnp.uint32)
        chip, core = me >> 1, me & 1
        positions = jnp.arange(seq)
        cos_tab, sin_tab = rotary_tables(positions, head_dim)
        cos_full = jnp.concatenate([cos_tab, cos_tab], axis=1)
        sin_full = jnp.concatenate([-sin_tab, sin_tab], axis=1)
        scale_all = lax.all_gather(ln_scale, 'm', axis=0)
        layers = w_gate.shape[0]
        heads = w_q.shape[2]

        def spread(w, e_axis, layer, same_col, same_row, c_index):
            f_axis = 1 - e_axis
            half = w.shape[1 + f_axis] // 2
            quarter = half // 2

            def take(at, size):
                starts, sizes = [jnp.uint32(layer), jnp.uint32(0), jnp.uint32(0)], list(w.shape[1:3])
                starts[1 + f_axis], sizes[f_axis] = at * size, size
                tail = w.shape[3:]
                starts += [jnp.uint32(0)] * len(tail)
                return lax.dynamic_slice(w, starts, [1] + sizes + list(tail))[0]

            other = swap_core(take(1 - core, half))
            other_at = lambda i: lax.dynamic_slice_in_dim(other, i * quarter, quarter, f_axis)
            mine_c = jnp.concatenate([take(2 * core + c_index, quarter), other_at(c_index)], axis=e_axis)
            other_c = jnp.concatenate([take(2 * core + (1 - c_index), quarter), other_at(1 - c_index)], axis=e_axis)
            from_row = same_row.send(other_c)
            return [mine_c, from_row, same_col.send(mine_c), same_col.send(from_row)]

        def spread_kv(w, same_col, same_row):
            from_row = same_row.send(w)
            mine = jnp.stack([w, from_row, same_col.send(w), same_col.send(from_row)])
            full = jnp.concatenate([mine, swap_core(mine)], axis=1)
            return [full[i] for i in range(4)]

        plans = []
        for layer in range(layers):
            same_col = pairings[layer % 2]
            same_row = pairings[(layer + 1) % 2]
            flipped = layer % 2
            c_index = ((chip + flipped) >> 1) & 1
            owners = tuple(chip ^ mask for mask in ((0, 3, 1, 2), (0, 1, 3, 2))[flipped])
            order = jnp.stack([2 * owner + (core ^ j) for owner in owners for j in range(2)]).astype(jnp.int32)
            args = (same_col, same_row, c_index)
            gate = spread(w_gate, 0, layer, *args)
            up = spread(w_up, 0, layer, *args)
            query_w = spread(jnp.swapaxes(w_q, 1, 2), 1, layer, *args)
            kv_w = spread_kv(jnp.concatenate([w_k[layer], w_v[layer]], axis=1), same_col, same_row)
            down = spread(w_down, 1, layer, *args)
            out_w = spread(w_o.reshape(layers, heads * head_dim, w_o.shape[-1]), 1, layer, *args)
            lens = jnp.stack([prompt_len, same_row.send(prompt_len)])
            lens = jnp.stack([lens, swap_core(lens)])
            plans.append((same_row, order, lens, gate, up, query_w, kv_w, down, out_w))

        hidden = [lax.optimization_barrier(x_in[c]) for c in range(rows)]
        k_layers = []
        v_layers = []
        for layer in range(layers):
            same_row, order, lens, gate, up, query_w, kv_w, down, out_w = plans[layer]
            k_rows, v_rows, following = [], [], []
            for c in range(rows):
                shared = same_row.send(hidden[c])
                pair = jnp.concatenate([hidden[c], shared], axis=0)
                mine = lax.all_gather(pair, 'm', axis=0)
                other = swap_core(mine)
                both, key_rows, val_rows = up_call(order, lens[:, :, c].reshape(-1), mine, other, scale_all[:, layer], cos_full, sin_full, gate, up, query_w, kv_w)
                k_rows.append(key_rows)
                v_rows.append(val_rows)
                keep, send = down_call(order, both, down, out_w)
                from_core = swap_core(send)
                ordered = (keep.astype(jnp.float32) + from_core.astype(jnp.float32)).astype(jnp.bfloat16)
                reduced = lax.psum_scatter(ordered, 'm', scatter_dimension=0)
                from_row = same_row.send(reduced[seq:])
                following.append((hidden[c].astype(jnp.float32) + (reduced[:seq].astype(jnp.float32) + from_row.astype(jnp.float32))).astype(jnp.bfloat16))
            hidden = following
            k_layers.append(jnp.stack(k_rows))
            v_layers.append(jnp.stack(v_rows))
        return jnp.stack(hidden), jnp.stack(k_layers), jnp.stack(v_layers)

    return jax.shard_map(device_program, mesh=mesh, in_specs=in_specs, out_specs=(row_spec, cache_spec, cache_spec), check_vma=False)
```
